512 devices in a mesh: uly: 8 (over y, core), blk: 64 (over x, z).
Axes of the slice: x: 4, y: 4, z: 16, core: 2. Of those that a mesh axis runs over, the one named last changes fastest.
Arguments:
- query_inputs: bfloat16 [65536, 2048], P(('blk', 'uly')), may hold values from -6 to 6
- key_inputs: bfloat16 [65536, 1024], P(('blk', 'uly')), may hold values from -6 to 6
- value_inputs: bfloat16 [65536, 1024], P(('blk', 'uly')), may hold values from -6 to 6
- forward_out: bfloat16 [65536, 2048], P(('blk', 'uly')), may hold values from -6 to 6
- output_gradient: bfloat16 [65536, 2048], P(('blk', 'uly')), may hold values from -4 to 4
- lse_parts: float32 [65536, 16, 2], P(('blk', 'uly')), may hold values from 3 to 247
- segment_ids: int32 [65536], P(('blk', 'uly')), may hold values from 0 to 127, never falling along the last dimension, each value on 1 to 2048 neighbouring positions
Outputs:
- query_grad: bfloat16 [65536, 2048], P(('blk', 'uly'))
- key_grad: bfloat16 [65536, 1024], P(('blk', 'uly'))
- value_grad: bfloat16 [65536, 1024], P(('blk', 'uly'))
The draws below stay inside these ranges and needn't reach their ends.
Inputs may be any that keep to these rules, and one draw needn't show every extreme that they name: `segment_ids`: never falls along the sequence; every document holds 1 to 2048 tokens, and some document exactly 2048.
All inputs are finite; a program needn't handle non-finite values.
Results may differ from the reference program's by a relative error of at most 0.0051.
Values may be sent and summed in bfloat16 or wider, within the bound.
A program may use at most 128 MiB of HBM per device.

```python
import math
import jax
import jax.numpy as jnp
import numpy as np
from jax import lax

HEAD_SIZE = 128
QUERY_HEADS = 16
KEY_VALUE_HEADS = 8
QBLOCK = 512
SEQUENCE_TOKENS = 65536
DOCUMENT_LIMIT = 2048
SEGS = 128


def draw_lse_parts(key, part):
    first_key = jax.random.fold_in(key, 0)
    shape_all = (SEQUENCE_TOKENS, QUERY_HEADS, 2)
    return jnp.clip(5.0 + 0.8 * jax.random.normal(first_key, shape_all, jnp.float32), 3.0, 7.0)


def shard_levels(key, dims, cuts, least, top_value):
    def one(dim, shards_of):
        draws = jax.random.uniform(jax.random.fold_in(jax.random.fold_in(key, 6), dim), (shards_of,), jnp.float32, least / len(cuts), top_value / len(cuts))
        return jnp.repeat(jnp.exp(draws), dims[dim] // shards_of).reshape((-1,) + (1,) * (len(dims) - dim - 1))

    loudness = one(*cuts[0])
    for cut in cuts[1:]:
        loudness = loudness * one(*cut)
    return loudness


def split_up(count, total, most, slope):
    loads = [(1 << 20) // math.isqrt(grade ** slope) + 1 for grade in range(2, count + 1)]
    rest, counts = total - most - (count - 1), [1] * (count - 1)
    while rest > 0:
        candidates = [i for i in range(count - 1) if counts[i] < most]
        pool, budget = sum([loads[i] for i in candidates]), rest
        for i in candidates:
            extra = min(most - counts[i], max(1, budget * loads[i] // pool), rest)
            counts[i] = counts[i] + extra
            rest = rest - extra
    return np.array([most] + counts)


def ragged_sizes(rng, number_of, total, bound, slope):
    if number_of == 2:
        one = jax.random.randint(rng, (), max(1, total - bound), min(bound, total - 1) + 1)
        return jnp.stack([one, total - one])
    sizes = jnp.asarray(split_up(number_of, total, bound, slope), jnp.int32)
    pairs = (number_of - 1) // 2
    donor, taker = sizes[1:1 + 2 * pairs:2], sizes[2:2 + 2 * pairs:2]
    room = jnp.minimum(donor - 1, bound - taker)
    passed = jax.random.randint(jax.random.fold_in(rng, 1), (pairs,), 0, 1 << 20) % (room + 1)
    sizes = sizes.at[1:1 + 2 * pairs:2].set(donor - passed).at[2:2 + 2 * pairs:2].set(taker + passed)
    return sizes[jax.random.permutation(jax.random.fold_in(rng, 2), number_of)]


def scatter_about(rng, extent, deviation, limit, cuts=(), kind=jnp.bfloat16):
    array = jax.random.normal(rng, extent, jnp.float32) * deviation
    if len(cuts) > 0:
        array = shard_levels(rng, extent, cuts, -0.22, 0.18) * array
    return jnp.clip(array, min=-limit, max=limit).astype(kind)


def setup_inputs(seed: int = 0) -> dict:
    keys = jax.random.split(jax.random.key(seed), 8)
    return {
        "query_inputs": scatter_about(keys[0], (SEQUENCE_TOKENS, QUERY_HEADS * HEAD_SIZE), 1.0, 6.0, ((0, 512),)),
        "key_inputs": scatter_about(keys[1], (SEQUENCE_TOKENS, KEY_VALUE_HEADS * HEAD_SIZE), 1.0, 6.0, ((0, 512),)),
        "value_inputs": scatter_about(keys[2], (SEQUENCE_TOKENS, KEY_VALUE_HEADS * HEAD_SIZE), 1.0, 6.0, ((0, 512),)),
        "forward_out": scatter_about(keys[3], (SEQUENCE_TOKENS, QUERY_HEADS * HEAD_SIZE), 0.5, 6.0, ((0, 512),)),
        "output_gradient": scatter_about(keys[4], (SEQUENCE_TOKENS, QUERY_HEADS * HEAD_SIZE), 0.25, 4.0, ((0, 512),)),
        "lse_parts": draw_lse_parts(jax.random.fold_in(keys[7], 71), 0),
        "segment_ids": jnp.searchsorted(jnp.cumsum(ragged_sizes(keys[6], SEGS, SEQUENCE_TOKENS, DOCUMENT_LIMIT, 2)), jnp.arange(SEQUENCE_TOKENS), side="right").astype(jnp.int32),
    }


def merge_parts(partials):
    highest = lax.optimization_barrier(jnp.max(partials, axis=-1))
    return highest + jnp.log(lax.optimization_barrier(jnp.sum(jnp.exp(partials - highest[..., None]), axis=-1)))

def round_trip(values_in):
    rounded = lax.optimization_barrier(values_in.astype(jnp.bfloat16))
    return rounded.astype(jnp.float32)

def reference(query_inputs, key_inputs, value_inputs, forward_out, output_gradient, lse_parts, segment_ids):
    token_count = query_inputs.shape[0]
    group_width = QUERY_HEADS // KEY_VALUE_HEADS
    score_scale = 1.0 / math.sqrt(HEAD_SIZE)
    rows_per_block = min(QBLOCK, token_count)
    lookback_span = DOCUMENT_LIMIT + rows_per_block
    logsumexp_rows = merge_parts(lse_parts)
    products = output_gradient.astype(jnp.float32) * forward_out.astype(jnp.float32)
    row_deltas = lax.optimization_barrier(jnp.sum(products.reshape(token_count, QUERY_HEADS, HEAD_SIZE), axis=-1))
    key_with_padding = jnp.pad(key_inputs, ((DOCUMENT_LIMIT, 0), (0, 0)))
    value_with_padding = jnp.pad(value_inputs, ((DOCUMENT_LIMIT, 0), (0, 0)))
    ids_padded = jnp.concatenate([jnp.full((DOCUMENT_LIMIT,), -1, jnp.int32), segment_ids.astype(jnp.int32)])

    def block_step(carried, block_index):
        key_gradient_running, value_gradient_running = carried
        leading_row = (block_index * rows_per_block).astype(jnp.int32)
        query_quad = lax.dynamic_slice_in_dim(query_inputs, leading_row, rows_per_block, 0).astype(jnp.float32).reshape(rows_per_block, KEY_VALUE_HEADS, group_width, HEAD_SIZE)
        gradient_quad = lax.dynamic_slice_in_dim(output_gradient, leading_row, rows_per_block, 0).astype(jnp.float32).reshape(rows_per_block, KEY_VALUE_HEADS, group_width, HEAD_SIZE)
        logsumexp_cube = lax.dynamic_slice_in_dim(logsumexp_rows, leading_row, rows_per_block, 0).reshape(rows_per_block, KEY_VALUE_HEADS, group_width).transpose(1, 2, 0)[..., None]
        delta_cube = lax.dynamic_slice_in_dim(row_deltas, leading_row, rows_per_block, 0).reshape(rows_per_block, KEY_VALUE_HEADS, group_width).transpose(1, 2, 0)[..., None]
        key_cube = lax.dynamic_slice_in_dim(key_with_padding, leading_row, lookback_span, 0).astype(jnp.float32).reshape(lookback_span, KEY_VALUE_HEADS, HEAD_SIZE)
        value_cube = lax.dynamic_slice_in_dim(value_with_padding, leading_row, lookback_span, 0).astype(jnp.float32).reshape(lookback_span, KEY_VALUE_HEADS, HEAD_SIZE)
        query_ids = lax.dynamic_slice_in_dim(segment_ids.astype(jnp.int32), leading_row, rows_per_block, 0)
        key_ids = lax.dynamic_slice_in_dim(ids_padded, leading_row, lookback_span, 0)
        query_pos = leading_row + DOCUMENT_LIMIT + jnp.arange(rows_per_block, dtype=jnp.int32)
        key_pos = leading_row + jnp.arange(lookback_span, dtype=jnp.int32)
        allowed = (key_pos[None, :] <= query_pos[:, None]) & (key_ids[None, :] == query_ids[:, None])
        scores = jnp.einsum('mhgd,nhd->hgmn', query_quad, key_cube) * score_scale
        weights = jnp.where(allowed, jnp.exp(scores - logsumexp_cube), 0.0)
        value_portion = jnp.einsum('hgmn,mhgd->nhd', round_trip(weights), gradient_quad)
        prob_grad = jnp.einsum('mhgd,nhd->hgmn', gradient_quad, value_cube)
        score_grad = round_trip(weights * (prob_grad - delta_cube))
        query_part = jnp.einsum('hgmn,nhd->mhgd', score_grad, key_cube) * score_scale
        key_portion = jnp.einsum('hgmn,mhgd->nhd', score_grad, query_quad) * score_scale
        key_window_rows = lax.dynamic_slice_in_dim(key_gradient_running, leading_row, lookback_span, 0) + key_portion.reshape(lookback_span, KEY_VALUE_HEADS * HEAD_SIZE)
        value_window_rows = lax.dynamic_slice_in_dim(value_gradient_running, leading_row, lookback_span, 0) + value_portion.reshape(lookback_span, KEY_VALUE_HEADS * HEAD_SIZE)
        key_gradient_running = lax.dynamic_update_slice_in_dim(key_gradient_running, key_window_rows, leading_row, 0)
        value_gradient_running = lax.dynamic_update_slice_in_dim(value_gradient_running, value_window_rows, leading_row, 0)
        return ((key_gradient_running, value_gradient_running), query_part.reshape(rows_per_block, QUERY_HEADS * HEAD_SIZE).astype(jnp.bfloat16))
    initial_running = (jnp.zeros((token_count + DOCUMENT_LIMIT, KEY_VALUE_HEADS * HEAD_SIZE), jnp.float32), jnp.zeros((token_count + DOCUMENT_LIMIT, KEY_VALUE_HEADS * HEAD_SIZE), jnp.float32))
    final_acc, query_blocks = lax.scan(block_step, initial_running, jnp.arange(token_count // rows_per_block, dtype=jnp.int32))
    query_grad = query_blocks.reshape(token_count, QUERY_HEADS * HEAD_SIZE)
    key_grad = final_acc[0][DOCUMENT_LIMIT:].astype(jnp.bfloat16)
    value_grad = final_acc[1][DOCUMENT_LIMIT:].astype(jnp.bfloat16)
    return (query_grad, key_grad, value_grad)
```

```python
import math

import jax
import jax.numpy as jnp
from jax import lax
from jax.experimental import pallas as pl
from jax.experimental.pallas import tpu as pltpu
from jax.sharding import PartitionSpec as P

D = 128
HEADS = 16
GROUPS = 8
TOK = 128
ROWS = TOK * GROUPS
CH = 256
NCH = ROWS // CH
QB = 512
LOG2E = math.log2(math.e)
SCALE = 1.0 / math.sqrt(D)
MESH = pl.DeviceIdType.MESH
F32 = jnp.float32
BF16 = jnp.bfloat16


def mo(value, unit):
    return pl.multiple_of(value, unit)


def kernel(
    q_in, k_in, v_in, o_in, g_in, lp_in, id_in,
    q_out, k_out, v_out,
    Q, G, KV, ST, IDT, IDR, IDC,
    o_s, g_s, st_src, id_src,
    DQ, ACC0, ACC1, ACC2,
    S2, R2, S1, R1, SO, SQ,
    in_send, in_recv, st_send, st_recv, id_send, id_recv,
    hop_send, hop_recv, ret_send, ret_recv,
    oq_send, oq_recv, okv_send, okv_recv, loc,
):
    me = lax.axis_index("uly")
    blk = lax.axis_index("blk")
    nblk = lax.axis_size("blk")
    nxt = lax.rem(blk + 1, nblk)
    prv = lax.rem(blk + nblk - 1, nblk)

    def peer(d):
        return lax.rem(me + d, GROUPS)

    def rcopy(src, dst, ss, rs, p, b):
        return pltpu.make_async_remote_copy(
            src_ref=src, dst_ref=dst, send_sem=ss, recv_sem=rs,
            device_id=(p, b), device_id_type=MESH,
        )

    cp_g = pltpu.make_async_copy(g_in, g_s, loc.at[0])
    cp_o = pltpu.make_async_copy(o_in, o_s, loc.at[1])
    cp_g.start()
    cp_o.start()
    idrow = id_in[...].astype(F32)
    id_src[...] = jnp.broadcast_to(idrow, (8, TOK))

    barrier = pltpu.get_barrier_semaphore()

    def greet(d, _):
        pl.semaphore_signal(barrier, inc=1, device_id=(peer(d), blk), device_id_type=MESH)
        return 0

    lax.fori_loop(1, GROUPS, greet, 0)
    pl.semaphore_signal(barrier, inc=1, device_id=(me, nxt), device_id_type=MESH)
    pl.semaphore_signal(barrier, inc=1, device_id=(me, prv), device_id_type=MESH)
    pl.semaphore_wait(barrier, GROUPS + 1)

    myrow = pl.ds(mo(me * TOK, TOK), TOK)

    def in_copy(kind, p, src_i):
        row = pl.ds(mo(src_i * TOK, TOK), TOK)
        if kind == 0:
            src, dst = k_in.at[:, pl.ds(mo(p * D, D), D)], KV.at[0, row, 0:D]
        elif kind == 1:
            src, dst = v_in.at[:, pl.ds(mo(p * D, D), D)], KV.at[0, row, D : 2 * D]
        elif kind == 2:
            src, dst = q_in.at[:, pl.ds(mo(p * 2 * D, D), 2 * D)], Q.at[row, :]
        else:
            src, dst = g_in.at[:, pl.ds(mo(p * 2 * D, D), 2 * D)], G.at[row, :]
        return src, dst

    def id_copy(p, src_i):
        return rcopy(id_src, IDT.at[src_i], id_send.at[p], id_recv.at[src_i], p, blk)

    def big_copy(kind, p, src_i):
        src, dst = in_copy(kind, p, src_i)
        return rcopy(src, dst, in_send.at[kind, p], in_recv.at[kind, src_i], p, blk)

    def st_copy(p, src_i):
        return rcopy(st_src.at[p], ST.at[src_i], st_send.at[p], st_recv.at[src_i], p, blk)

    def each_peer(f):
        def body(d, _):
            f(peer(d))
            return 0

        lax.fori_loop(1, GROUPS, body, 0)

    def send_ids_kv(p):
        id_copy(p, me).start()
        big_copy(0, p, me).start()
        big_copy(1, p, me).start()

    def send_qg(p):
        big_copy(2, p, me).start()
        big_copy(3, p, me).start()

    each_peer(send_ids_kv)
    own = []
    for kind in range(4):
        src, dst = in_copy(kind, me, me)
        own.append(pltpu.make_async_copy(src, dst, loc.at[2 + kind]))
        own[-1].start()
    each_peer(send_qg)
    IDT[me] = id_src[...]

    a, b = lp_in[:, 0, :], lp_in[:, 1, :]
    top = jnp.maximum(a, b)
    lse = (top + jnp.log(jnp.exp(a - top) + jnp.exp(b - top))) * LOG2E
    cp_g.wait()
    cp_o.wait()
    lane = lax.broadcasted_iota(jnp.int32, (TOK, D), 1)

    def delta_step(h, acc):
        cols = pl.ds(mo(h * D, D), D)
        total = jnp.sum(g_s[:, cols].astype(F32) * o_s[:, cols].astype(F32), axis=1, keepdims=True)
        return jnp.where(lane == h, total, acc)

    deltas = lax.fori_loop(0, HEADS, delta_step, jnp.zeros((TOK, D), F32)).T
    for g in range(GROUPS):
        st_src[g] = jnp.concatenate(
            [lse[2 * g : 2 * g + 2], deltas[2 * g : 2 * g + 2], jnp.zeros((4, TOK), F32)], axis=0
        )

    each_peer(lambda p: id_copy(me, p).wait_recv())
    IDR[0] = IDT[:, 0, :]
    each_peer(lambda p: st_copy(p, me).start())
    ST[me] = st_src[me]

    def hop_copy(slot, c):
        rows = pl.ds(mo(c * CH, CH), CH)
        return rcopy(
            KV.at[slot, rows, :], KV.at[slot + 1, rows, :],
            hop_send.at[slot, c], hop_recv.at[slot, c], me, nxt,
        )

    def ids_hop(slot):
        return rcopy(
            IDR.at[slot], IDR.at[slot + 1], hop_send.at[slot, NCH], hop_recv.at[slot, NCH], me, nxt
        )

    def columns_of(slot):
        for s in range(GROUPS):
            tile = jnp.broadcast_to(IDR[slot, s : s + 1, :], (TOK, TOK))
            IDC[slot, s * TOK : (s + 1) * TOK, :] = tile.T

    def wait_kv(p):
        big_copy(0, me, p).wait_recv()
        big_copy(1, me, p).wait_recv()

    each_peer(wait_kv)
    own[0].wait()
    own[1].wait()
    ids_hop(0).start()
    for c in range(NCH):
        hop_copy(0, c).start()
    columns_of(0)
    ids_hop(0).wait_recv()
    ids_hop(1).start()
    columns_of(1)
    for c in range(NCH):
        hop_copy(0, c).wait_recv()
        hop_copy(1, c).start()

    def wait_qg(p):
        big_copy(2, me, p).wait_recv()
        big_copy(3, me, p).wait_recv()
        st_copy(me, p).wait_recv()

    each_peer(wait_qg)
    own[2].wait()
    own[3].wait()

    def tile(slot, c, qb, acc, causal):
        krows = pl.ds(mo(c * CH, CH), CH)
        qrows = pl.ds(mo(qb * QB, QB), QB)
        kt = KV[slot, krows, 0:D]
        vt = KV[slot, krows, D : 2 * D]
        idk = IDC[slot, krows, :]
        nq = QB // TOK
        first = qb * nq

        def row(r):
            return jnp.concatenate([ST[first + i, r : r + 1, :] for i in range(nq)], axis=1)

        idq = jnp.concatenate([IDR[0, pl.ds(first + i, 1), :] for i in range(nq)], axis=1)
        allowed = jnp.concatenate([idk] * nq, axis=1) == idq
        if causal:
            kpos = lax.broadcasted_iota(jnp.int32, (CH, QB), 0) + c * CH
            qpos = lax.broadcasted_iota(jnp.int32, (CH, QB), 1) + qb * QB
            allowed = allowed & (kpos <= qpos)
        dk = jnp.zeros((CH, D), F32)
        dv = jnp.zeros((CH, D), F32)
        for h in range(2):
            cols = slice(h * D, (h + 1) * D)
            qt = Q[qrows, cols]
            gt = G[qrows, cols]
            s = lax.dot_general(kt, qt, (((1,), (1,)), ((), ())), preferred_element_type=F32)
            w = jnp.where(allowed, jnp.exp2(s * (SCALE * LOG2E) - row(h)), 0.0)
            dp = lax.dot_general(vt, gt, (((1,), (1,)), ((), ())), preferred_element_type=F32)
            sg = (w * (dp - row(2 + h))).astype(BF16)
            dv = dv + jnp.dot(w.astype(BF16), gt, preferred_element_type=F32)
            dk = dk + jnp.dot(sg, qt, preferred_element_type=F32)
            DQ[qrows, cols] += lax.dot_general(
                sg, kt, (((0,), (0,)), ((), ())), preferred_element_type=F32
            )
        acc[krows, 0:D] += dk
        acc[krows, D : 2 * D] += dv

    DQ[...] = jnp.zeros_like(DQ)
    ACC0[...] = jnp.zeros_like(ACC0)
    ACC1[...] = jnp.zeros_like(ACC1)
    ACC2[...] = jnp.zeros_like(ACC2)

    def own_chunk(c, _):
        lax.fori_loop((c * CH) // QB, ROWS // QB, lambda qb, _: (tile(0, c, qb, ACC0, True), 0)[1], 0)
        return 0

    lax.fori_loop(0, NCH, own_chunk, 0)
    ids_hop(1).wait_recv()
    columns_of(2)

    def ret_copy(stage, c):
        rows = pl.ds(mo(c * CH, CH), CH)
        src, dst = (S2, R2) if stage == 0 else (S1, R1)
        return rcopy(
            src.at[rows, :], dst.at[rows, :], ret_send.at[stage, c], ret_recv.at[stage, c], me, prv
        )

    def pass_on(c):
        rows = pl.ds(mo(c * CH, CH), CH)
        ret_copy(0, c).wait_recv()
        S1[rows, :] = (ACC1[rows, :] + R2[rows, :].astype(F32)).astype(BF16)
        ret_copy(1, c).start()

    scales = jnp.where(lax.broadcasted_iota(jnp.int32, (CH, 2 * D), 1) < D, SCALE, 1.0)

    def hop_chunk(c, _):
        rows = pl.ds(mo(c * CH, CH), CH)
        hop_copy(1, c).wait_recv()
        trips = (c * CH) // QB + 1
        lax.fori_loop(0, trips, lambda qb, _: (tile(2, c, qb, ACC2, False), 0)[1], 0)
        S2[rows, :] = (ACC2[rows, :] * scales).astype(BF16)
        ret_copy(0, c).start()
        lax.fori_loop(0, ROWS // QB, lambda qb, _: (tile(1, c, qb, ACC1, False), 0)[1], 0)
        ACC1[rows, :] = ACC1[rows, :] * scales

        @pl.when(c > 0)
        def _():
            pass_on(c - 1)

        return 0

    lax.fori_loop(0, NCH, hop_chunk, 0)

    def oq_copy(p, src_i):
        return rcopy(
            SQ.at[pl.ds(mo(p * TOK, TOK), TOK), :],
            q_out.at[:, pl.ds(mo(src_i * 2 * D, D), 2 * D)],
            oq_send.at[p], oq_recv.at[src_i], p, blk,
        )

    SQ[...] = (DQ[...] * SCALE).astype(BF16)
    each_peer(lambda p: oq_copy(p, me).start())
    own_q = pltpu.make_async_copy(
        SQ.at[myrow, :], q_out.at[:, pl.ds(mo(me * 2 * D, D), 2 * D)], loc.at[6]
    )
    own_q.start()
    pass_on(NCH - 1)

    def okv_copy(kind, p, src_i):
        src = SO.at[pl.ds(mo(p * TOK, TOK), TOK), kind * D : (kind + 1) * D]
        dst = (k_out, v_out)[kind].at[:, pl.ds(mo(src_i * D, D), D)]
        return rcopy(src, dst, okv_send.at[kind, p], okv_recv.at[kind, src_i], p, blk)

    def own_kv(kind):
        src = SO.at[myrow, kind * D : (kind + 1) * D]
        dst = (k_out, v_out)[kind].at[:, pl.ds(mo(me * D, D), D)]
        return pltpu.make_async_copy(src, dst, loc.at[7 + kind])

    per = CH // TOK

    def out_chunk(c, _):
        rows = pl.ds(mo(c * CH, CH), CH)
        ret_copy(1, c).wait_recv()
        SO[rows, :] = (ACC0[rows, :] * scales + R1[rows, :].astype(F32)).astype(BF16)
        for i in range(per):
            p = c * per + i

            @pl.when(p != me)
            def _():
                okv_copy(0, p, me).start()
                okv_copy(1, p, me).start()

            @pl.when(p == me)
            def _():
                own_kv(0).start()
                own_kv(1).start()

        return 0

    lax.fori_loop(0, NCH, out_chunk, 0)

    def drain_sends(p):
        id_copy(p, me).wait_send()
        for kind in range(4):
            big_copy(kind, p, me).wait_send()
        st_copy(p, me).wait_send()
        oq_copy(p, me).wait_send()
        okv_copy(0, p, me).wait_send()
        okv_copy(1, p, me).wait_send()

    each_peer(drain_sends)
    for slot in range(2):
        ids_hop(slot).wait_send()
    for stage in range(2):
        for c in range(NCH):
            hop_copy(stage, c).wait_send()
            ret_copy(stage, c).wait_send()

    def drain_recvs(p):
        oq_copy(me, p).wait_recv()
        okv_copy(0, me, p).wait_recv()
        okv_copy(1, me, p).wait_recv()

    each_peer(drain_recvs)
    own_q.wait()
    own_kv(0).wait()
    own_kv(1).wait()


def per_device(q, k, v, o, g, lp, ids):
    lp = lp.transpose(1, 2, 0)
    ids = ids.reshape(1, TOK)
    any_spec = pl.BlockSpec(memory_space=pl.ANY)
    vmem = pl.BlockSpec(memory_space=pltpu.VMEM)
    dma = pltpu.SemaphoreType.DMA
    scratch = [
        pltpu.VMEM((ROWS, 2 * D), BF16),
        pltpu.VMEM((ROWS, 2 * D), BF16),
        pltpu.VMEM((3, ROWS, 2 * D), BF16),
        pltpu.VMEM((GROUPS, 8, TOK), F32),
        pltpu.VMEM((GROUPS, 8, TOK), F32),
        pltpu.VMEM((3, GROUPS, TOK), F32),
        pltpu.VMEM((3, ROWS, TOK), F32),
        pltpu.VMEM((TOK, HEADS * D), BF16),
        pltpu.VMEM((TOK, HEADS * D), BF16),
        pltpu.VMEM((GROUPS, 8, TOK), F32),
        pltpu.VMEM((8, TOK), F32),
        pltpu.VMEM((ROWS, 2 * D), F32),
        pltpu.VMEM((ROWS, 2 * D), F32),
        pltpu.VMEM((ROWS, 2 * D), F32),
        pltpu.VMEM((ROWS, 2 * D), F32),
        pltpu.VMEM((ROWS, 2 * D), BF16),
        pltpu.VMEM((ROWS, 2 * D), BF16),
        pltpu.VMEM((ROWS, 2 * D), BF16),
        pltpu.VMEM((ROWS, 2 * D), BF16),
        pltpu.VMEM((ROWS, 2 * D), BF16),
        pltpu.VMEM((ROWS, 2 * D), BF16),
        dma((4, GROUPS)), dma((4, GROUPS)),
        dma((GROUPS,)), dma((GROUPS,)),
        dma((GROUPS,)), dma((GROUPS,)),
        dma((2, NCH + 1)), dma((2, NCH + 1)),
        dma((2, NCH)), dma((2, NCH)),
        dma((GROUPS,)), dma((GROUPS,)),
        dma((2, GROUPS)), dma((2, GROUPS)),
        dma((9,)),
    ]
    return pl.pallas_call(
        kernel,
        out_shape=(
            jax.ShapeDtypeStruct((TOK, HEADS * D), BF16),
            jax.ShapeDtypeStruct((TOK, GROUPS * D), BF16),
            jax.ShapeDtypeStruct((TOK, GROUPS * D), BF16),
        ),
        in_specs=[any_spec] * 5 + [vmem, vmem],
        out_specs=(any_spec,) * 3,
        scratch_shapes=scratch,
        compiler_params=pltpu.CompilerParams(
            collective_id=0, has_side_effects=True, vmem_limit_bytes=48 * 1024 * 1024
        ),
        name="attention_backward",
    )(q, k, v, o, g, lp, ids)


def solution(mesh):
    tokens = ("blk", "uly")
    row = P(tokens, None)
    in_specs = (row, row, row, row, row, P(tokens, None, None), P(tokens))
    return jax.shard_map(
        per_device, mesh=mesh, in_specs=in_specs, out_specs=(row, row, row), check_vma=False
    )
```

```python
import math

import jax
import jax.numpy as jnp
from jax import lax
from jax.experimental import pallas as pl
from jax.experimental.pallas import tpu as pltpu
from jax.sharding import PartitionSpec as P

D = 128
HEADS = 16
GROUPS = 8
TOK = 128
ROWS = TOK * GROUPS
CH = 256
NCH = ROWS // CH
NY = 4
QB = 512
LOG2E = math.log2(math.e)
SCALE = 1.0 / math.sqrt(D)
MESH = pl.DeviceIdType.MESH
F32 = jnp.float32
BF16 = jnp.bfloat16


def mo(value, unit):
    return pl.multiple_of(value, unit)


def kernel(
    q_in, k_in, v_in, o_in, g_in, lp_in, id_in,
    q_out, k_out, v_out,
    Q, G, KV, ST, IDT, IDR, IDC,
    o_s, g_s, q_s, st_src, id_src, SKV, PKV, PQ, PG,
    DQ, ACC0, ACC1, ACC2,
    S2, R2, S1, R1, SO, SQ, XQ, XKV,
    loc, skv_sem, d2d_send, d2d_recv, yo_send, yo_recv,
    st_send, st_recv, id_send, id_recv,
    hop_send, hop_recv, ret_send, ret_recv,
    oq_send, oq_recv, okv_send, okv_recv, fwd_send, fwd_recv, lout,
):
    me = lax.axis_index("uly")
    blk = lax.axis_index("blk")
    nblk = lax.axis_size("blk")
    nxt = lax.rem(blk + 1, nblk)
    prv = lax.rem(blk + nblk - 1, nblk)
    y = me // 2
    core = lax.rem(me, 2)
    mate = me + 1 - 2 * core

    def rcopy(src, dst, ss, rs, p, b):
        return pltpu.make_async_remote_copy(
            src_ref=src, dst_ref=dst, send_sem=ss, recv_sem=rs,
            device_id=(p, b), device_id_type=MESH,
        )

    def peer(d):
        return lax.rem(me + d, GROUPS)

    def each_peer(f):
        def body(d, _):
            f(peer(d))
            return 0

        lax.fori_loop(1, GROUPS, body, 0)

    pair = y // 2

    def chip(k):
        step = k + (k // 2) * (5 - 2 * k)
        return lax.rem(y + (1 - 2 * lax.rem(y, 2)) * step + NY, NY)

    def rows_of(u):
        return pl.ds(mo(u * TOK, TOK), TOK)

    def chunk(c):
        return pl.ds(mo(c * CH, CH), CH)

    def wide(g):
        return pl.ds(mo(g * 2 * D, 2 * D), 2 * D)

    def narrow(g):
        return pl.ds(mo(g * D, D), D)

    cp_g = pltpu.make_async_copy(g_in, g_s, loc.at[0])
    cp_o = pltpu.make_async_copy(o_in, o_s, loc.at[1])
    cp_q = pltpu.make_async_copy(q_in, q_s, loc.at[6])

    def stage_kv(g):
        return (
            pltpu.make_async_copy(k_in.at[:, narrow(g)], SKV.at[g, :, 0:D], skv_sem.at[0, g]),
            pltpu.make_async_copy(v_in.at[:, narrow(g)], SKV.at[g, :, D : 2 * D], skv_sem.at[1, g]),
        )

    own = [
        pltpu.make_async_copy(k_in.at[:, narrow(me)], KV.at[0, rows_of(me), 0:D], loc.at[2]),
        pltpu.make_async_copy(v_in.at[:, narrow(me)], KV.at[0, rows_of(me), D : 2 * D], loc.at[3]),
        pltpu.make_async_copy(q_in.at[:, wide(me)], Q.at[rows_of(me), :], loc.at[4]),
        pltpu.make_async_copy(g_in.at[:, wide(me)], G.at[rows_of(me), :], loc.at[5]),
    ]

    barrier = pltpu.get_barrier_semaphore()

    def greet(d, _):
        pl.semaphore_signal(barrier, inc=1, device_id=(peer(d), blk), device_id_type=MESH)
        return 0

    lax.fori_loop(1, GROUPS, greet, 0)
    pl.semaphore_signal(barrier, inc=1, device_id=(me, nxt), device_id_type=MESH)
    pl.semaphore_signal(barrier, inc=1, device_id=(me, prv), device_id_type=MESH)

    def stage_step(g, _):
        for cp in stage_kv(g):
            cp.start()
        return 0

    lax.fori_loop(0, GROUPS, stage_step, 0)
    for cp in own:
        cp.start()
    cp_q.start()
    cp_g.start()
    cp_o.start()
    id_src[...] = jnp.broadcast_to(id_in[...].astype(F32), (8, TOK))

    def stage_wait(g, _):
        for cp in stage_kv(g):
            cp.wait()
        return 0

    lax.fori_loop(0, GROUPS, stage_wait, 0)
    pl.semaphore_wait(barrier, GROUPS + 1)

    def mate_copy(kind, t, here, there, same):
        g = 2 * t + lax.rem(there, 2)
        src = (SKV.at[g], q_s.at[:, wide(g)], g_s.at[:, wide(g)])[kind]
        if same:
            dst = (KV.at[0, rows_of(here), :], Q.at[rows_of(here), :], G.at[rows_of(here), :])[kind]
        else:
            dst = (PKV, PQ, PG)[kind].at[t]
        return rcopy(src, dst, d2d_send.at[kind, t], d2d_recv.at[kind, t], mate, blk)

    def mate_send(kind, k):
        return mate_copy(kind, chip(k), me, mate, k == 0)

    def mate_recv(kind, k):
        return mate_copy(kind, chip(k), mate, me, k == 0)

    for k in range(NY):
        mate_send(0, k).start()

    def id_copy(p, src_i):
        return rcopy(id_src, IDT.at[src_i], id_send.at[p], id_recv.at[src_i], p, blk)

    def st_copy(p, src_i):
        return rcopy(st_src.at[p], ST.at[src_i], st_send.at[p], st_recv.at[src_i], p, blk)

    each_peer(lambda p: id_copy(p, me).start())

    def y_copy(kind, part, t, s):
        g = 2 * t + core
        u = 2 * s + (core if part == 0 else 1 - core)
        if part == 0:
            src = (SKV.at[g], q_s.at[:, wide(g)], g_s.at[:, wide(g)])[kind]
        else:
            src = (PKV, PQ, PG)[kind].at[t]
        dst = (KV.at[0, rows_of(u), :], Q.at[rows_of(u), :], G.at[rows_of(u), :])[kind]
        return rcopy(
            src, dst, yo_send.at[kind, part, t], yo_recv.at[kind, part, s], g, blk
        )

    def hop_copy(slot, c):
        rows = chunk(c)
        return rcopy(
            KV.at[slot, rows, :], KV.at[slot + 1, rows, :],
            hop_send.at[slot, c], hop_recv.at[slot, c], me, nxt,
        )

    def ids_hop(slot):
        return rcopy(
            IDR.at[slot], IDR.at[slot + 1], hop_send.at[slot, NCH], hop_recv.at[slot, NCH], me, nxt
        )

    for k in range(1, NY):
        y_copy(0, 0, chip(k), y).start()
    cp_q.wait()
    cp_g.wait()
    for kind in (1, 2):
        for k in range(NY):
            mate_send(kind, k).start()
    own[0].wait()
    own[1].wait()
    mate_recv(0, 0).wait_recv()
    hop_copy(0, chip(0)).start()
    for k in range(1, NY):
        mate_recv(0, k).wait_recv()
        y_copy(0, 1, chip(k), y).start()
    for near in ((1, 2), (3,)):
        for k in near:
            for kind in (1, 2):
                y_copy(kind, 0, chip(k), y).start()
        for k in near:
            for kind in (1, 2):
                mate_recv(kind, k).wait_recv()
                y_copy(kind, 1, chip(k), y).start()

    IDT[me] = id_src[...]
    each_peer(lambda p: id_copy(me, p).wait_recv())
    IDR[0] = IDT[:, 0, :]

    def columns_of(slot):
        for s in range(GROUPS):
            tile = jnp.broadcast_to(IDR[slot, s : s + 1, :], (TOK, TOK))
            IDC[slot, s * TOK : (s + 1) * TOK, :] = tile.T

    def wait_kv(k):
        y_copy(0, 0, y, chip(k)).wait_recv()
        y_copy(0, 1, y, chip(k)).wait_recv()

    wait_kv(1)
    ids_hop(0).start()
    hop_copy(0, chip(1)).start()

    a, b = lp_in[:, 0, :], lp_in[:, 1, :]
    top = jnp.maximum(a, b)
    lse = (top + jnp.log(jnp.exp(a - top) + jnp.exp(b - top))) * LOG2E
    cp_o.wait()
    lane = lax.broadcasted_iota(jnp.int32, (TOK, D), 1)

    def delta_step(h, acc):
        cols = narrow(h)
        total = jnp.sum(g_s[:, cols].astype(F32) * o_s[:, cols].astype(F32), axis=1, keepdims=True)
        return jnp.where(lane == h, total, acc)

    deltas = lax.fori_loop(0, HEADS, delta_step, jnp.zeros((TOK, D), F32)).T
    for g in range(GROUPS):
        st_src[g] = jnp.concatenate(
            [lse[2 * g : 2 * g + 2], deltas[2 * g : 2 * g + 2], jnp.zeros((4, TOK), F32)], axis=0
        )
    ST[me] = st_src[me]
    each_peer(lambda p: st_copy(p, me).start())

    hop_copy(0, chip(0)).wait_recv()
    hop_copy(1, chip(0)).start()
    wait_kv(2)
    hop_copy(0, chip(2)).start()
    ids_hop(0).wait_recv()
    ids_hop(1).start()
    hop_copy(0, chip(1)).wait_recv()
    hop_copy(1, chip(1)).start()
    wait_kv(3)
    hop_copy(0, chip(3)).start()

    columns_of(0)
    columns_of(1)
    DQ[...] = jnp.zeros_like(DQ)
    ACC0[...] = jnp.zeros_like(ACC0)
    ACC1[...] = jnp.zeros_like(ACC1)
    ACC2[...] = jnp.zeros_like(ACC2)

    def tile(slot, c, qb, acc, causal, depth):
        krows = pl.ds(mo(c * depth, depth), depth)
        qrows = pl.ds(mo(qb * QB, QB), QB)
        kt = KV[slot, krows, 0:D]
        vt = KV[slot, krows, D : 2 * D]
        idk = IDC[slot, krows, :]
        nq = QB // TOK
        first = qb * nq

        def row(r):
            return jnp.concatenate([ST[first + i, r : r + 1, :] for i in range(nq)], axis=1)

        idq = jnp.concatenate([IDR[0, pl.ds(first + i, 1), :] for i in range(nq)], axis=1)
        allowed = jnp.concatenate([idk] * nq, axis=1) == idq
        if causal:
            kpos = lax.broadcasted_iota(jnp.int32, (depth, QB), 0) + c * depth
            qpos = lax.broadcasted_iota(jnp.int32, (depth, QB), 1) + qb * QB
            allowed = allowed & (kpos <= qpos)
        dk = jnp.zeros((depth, D), F32)
        dv = jnp.zeros((depth, D), F32)
        turned = kt.T
        for h in range(2):
            cols = slice(h * D, (h + 1) * D)
            qt = Q[qrows, cols]
            gt = G[qrows, cols]
            s = lax.dot_general(kt, qt, (((1,), (1,)), ((), ())), preferred_element_type=F32)
            w = jnp.where(allowed, jnp.exp2(s * (SCALE * LOG2E) - row(h)), 0.0)
            dp = lax.dot_general(vt, gt, (((1,), (1,)), ((), ())), preferred_element_type=F32)
            sg = (w * (dp - row(2 + h))).astype(BF16)
            dv = dv + jnp.dot(w.astype(BF16), gt, preferred_element_type=F32)
            dk = dk + jnp.dot(sg, qt, preferred_element_type=F32)
            DQ[cols, qrows] += jnp.dot(turned, sg, preferred_element_type=F32)
        acc[krows, 0:D] += dk
        acc[krows, D : 2 * D] += dv

    def wait_qg(k):
        for kind in (1, 2):
            y_copy(kind, 0, y, chip(k)).wait_recv()
            y_copy(kind, 1, y, chip(k)).wait_recv()

    def own_tiles(qb, count):
        lax.fori_loop(0, count, lambda c, _: (tile(0, c, qb, ACC0, True, QB), 0)[1], 0)

    each_peer(lambda p: st_copy(me, p).wait_recv())
    own[2].wait()
    own[3].wait()
    mate_recv(1, 0).wait_recv()
    mate_recv(2, 0).wait_recv()
    wait_qg(1)
    own_tiles(pair, pair + 1)
    hop_copy(0, chip(2)).wait_recv()
    hop_copy(1, chip(2)).start()
    wait_qg(2)
    wait_qg(3)
    ids_hop(1).wait_recv()
    columns_of(2)

    def ret_copy(stage, c):
        rows = chunk(c)
        src, dst = (S2, R2) if stage == 0 else (S1, R1)
        return rcopy(
            src.at[rows, :], dst.at[rows, :], ret_send.at[stage, c], ret_recv.at[stage, c], me, prv
        )

    scales = jnp.where(lax.broadcasted_iota(jnp.int32, (CH, 2 * D), 1) < D, SCALE, 1.0)

    def hop_two(c):
        hop_copy(1, c).wait_recv()
        trips = (c * CH) // QB + 1
        lax.fori_loop(0, trips, lambda qb, _: (tile(2, c, qb, ACC2, False, CH), 0)[1], 0)
        S2[chunk(c), :] = (ACC2[chunk(c), :] * scales).astype(BF16)
        ret_copy(0, c).start()

    def pass_on(c):
        ret_copy(0, c).wait_recv()
        S1[chunk(c), :] = (ACC1[chunk(c), :] * scales + R2[chunk(c), :].astype(F32)).astype(BF16)
        ret_copy(1, c).start()

    def hop_one(half):
        lax.fori_loop(0, ROWS // QB, lambda qb, _: (tile(1, half, qb, ACC1, False, QB), 0)[1], 0)

    def okv_copy(t, s):
        return rcopy(
            SO.at[chunk(t), :], XKV.at[s], okv_send.at[t], okv_recv.at[s], 2 * t + core, blk
        )

    def oq_copy(t, s):
        return rcopy(
            SQ.at[chunk(t), :], XQ.at[s], oq_send.at[t], oq_recv.at[s], 2 * t + core, blk
        )

    def total(c):
        ret_copy(1, c).wait_recv()
        return (ACC0[chunk(c), :] * scales + R1[chunk(c), :].astype(F32)).astype(BF16)

    def out_chunk(k):
        c = chip(k)
        SO[chunk(c), :] = total(c)
        okv_copy(c, y).start()

    def round_trip(j, _):
        hop_two(chip(j))

        @pl.when(j == 0)
        def _():
            hop_copy(0, chip(3)).wait_recv()
            hop_copy(1, chip(3)).start()

        @pl.when(lax.rem(j, 2) == 1)
        def _():
            own_tiles(1 - pair, (2 - pair) * ((3 - j) // 2))
            hop_one(pair + (1 - 2 * pair) * (j // 2))
            pass_on(chip(j - 1))
            pass_on(chip(j))

        return 0

    lax.fori_loop(0, NCH, round_trip, 0)
    out_chunk(1)

    mine = pl.ds(mo(core * TOK, TOK), TOK)
    theirs = pl.ds(mo((1 - core) * TOK, TOK), TOK)

    def forward(s, kind, owner):
        g = 2 * s + lax.rem(owner, 2)
        if kind == 0:
            src, dst = XQ.at[s, theirs, :], q_out.at[:, wide(g)]
        elif kind == 1:
            src, dst = XKV.at[s, theirs, 0:D], k_out.at[:, narrow(g)]
        else:
            src, dst = XKV.at[s, theirs, D : 2 * D], v_out.at[:, narrow(g)]
        return rcopy(src, dst, fwd_send.at[kind, s], fwd_recv.at[kind, s], mate, blk)

    def keep(s, kind):
        g = 2 * s + core
        if kind == 0:
            src, dst = XQ.at[s, mine, :], q_out.at[:, wide(g)]
        elif kind == 1:
            src, dst = XKV.at[s, mine, 0:D], k_out.at[:, narrow(g)]
        else:
            src, dst = XKV.at[s, mine, D : 2 * D], v_out.at[:, narrow(g)]
        return pltpu.make_async_copy(src, dst, lout.at[kind, s])

    def deliver(s, kind):
        forward(s, kind, me).start()
        keep(s, kind).start()

    def turn(c):
        return (DQ[:, chunk(c)] * SCALE).T.astype(BF16)

    def send_q(k, _):
        c = chip(k)
        SQ[chunk(c), :] = turn(c)
        oq_copy(c, y).start()
        return 0

    lax.fori_loop(1, NY, send_q, 0)
    XKV[y] = total(y)
    deliver(y, 1)
    deliver(y, 2)
    XQ[y] = turn(y)
    deliver(y, 0)
    out_chunk(2)
    out_chunk(3)

    def arrivals(k, _):
        s = chip(k)
        oq_copy(y, s).wait_recv()
        deliver(s, 0)
        return 0

    lax.fori_loop(1, NY, arrivals, 0)

    def arrivals_kv(k, _):
        s = chip(k)
        okv_copy(y, s).wait_recv()
        deliver(s, 1)
        deliver(s, 2)
        return 0

    lax.fori_loop(1, NY, arrivals_kv, 0)

    def drain_small(p):
        id_copy(p, me).wait_send()
        st_copy(p, me).wait_send()

    each_peer(drain_small)
    for slot in range(2):
        ids_hop(slot).wait_send()
    for stage in range(2):
        for c in range(NCH):
            hop_copy(stage, c).wait_send()
            ret_copy(stage, c).wait_send()
    for k in range(NY):
        for kind in range(3):
            mate_send(kind, k).wait_send()
            if k > 0:
                y_copy(kind, 0, chip(k), y).wait_send()
                y_copy(kind, 1, chip(k), y).wait_send()
        if k > 0:
            oq_copy(chip(k), y).wait_send()
            okv_copy(chip(k), y).wait_send()

    def drain_out(s, _):
        for kind in range(3):
            forward(s, kind, me).wait_send()
            keep(s, kind).wait()
            forward(s, kind, mate).wait_recv()
        return 0

    lax.fori_loop(0, NY, drain_out, 0)


def publish(q_in, k_in, v_in, q_out, k_out, v_out, q_s, k_s, v_s, read, write):
    moves = ((q_in, q_s, q_out), (k_in, k_s, k_out), (v_in, v_s, v_out))
    reads = [pltpu.make_async_copy(a, b, read.at[i]) for i, (a, b, _) in enumerate(moves)]
    writes = [pltpu.make_async_copy(b, c, write.at[i]) for i, (_, b, c) in enumerate(moves)]
    for cp in reads:
        cp.start()
    for cp, back in zip(reads, writes):
        cp.wait()
        back.start()
    for cp in writes:
        cp.wait()


def per_device(q, k, v, o, g, lp, ids):
    lp = lp.transpose(1, 2, 0)
    ids = ids.reshape(1, TOK)
    any_spec = pl.BlockSpec(memory_space=pl.ANY)
    vmem = pl.BlockSpec(memory_space=pltpu.VMEM)
    dma = pltpu.SemaphoreType.DMA
    slab = pltpu.VMEM((ROWS, 2 * D), BF16)
    acc = pltpu.VMEM((ROWS, 2 * D), F32)
    block = pltpu.VMEM((NY, TOK, 2 * D), BF16)
    scratch = [
        slab,
        slab,
        pltpu.VMEM((3, ROWS, 2 * D), BF16),
        pltpu.VMEM((GROUPS, 8, TOK), F32),
        pltpu.VMEM((GROUPS, 8, TOK), F32),
        pltpu.VMEM((3, GROUPS, TOK), F32),
        pltpu.VMEM((3, ROWS, TOK), F32),
        pltpu.VMEM((TOK, HEADS * D), BF16),
        pltpu.VMEM((TOK, HEADS * D), BF16),
        pltpu.VMEM((TOK, HEADS * D), BF16),
        pltpu.VMEM((GROUPS, 8, TOK), F32),
        pltpu.VMEM((8, TOK), F32),
        pltpu.VMEM((GROUPS, TOK, 2 * D), BF16),
        block, block, block,
        pltpu.VMEM((2 * D, ROWS), F32),
        acc, acc, acc,
        slab, slab, slab, slab, slab, slab,
        pltpu.VMEM((NY, CH, 2 * D), BF16),
        pltpu.VMEM((NY, CH, 2 * D), BF16),
        dma((7,)), dma((2, GROUPS)),
        dma((3, NY)), dma((3, NY)),
        dma((3, 2, NY)), dma((3, 2, NY)),
        dma((GROUPS,)), dma((GROUPS,)),
        dma((GROUPS,)), dma((GROUPS,)),
        dma((2, NCH + 1)), dma((2, NCH + 1)),
        dma((2, NCH)), dma((2, NCH)),
        dma((NY,)), dma((NY,)), dma((NY,)), dma((NY,)),
        dma((3, NY)), dma((3, NY)), dma((3, NY)),
    ]
    shapes = (
        jax.ShapeDtypeStruct((TOK, HEADS * D), BF16),
        jax.ShapeDtypeStruct((TOK, GROUPS * D), BF16),
        jax.ShapeDtypeStruct((TOK, GROUPS * D), BF16),
    )
    grads = pl.pallas_call(
        kernel,
        out_shape=shapes,
        in_specs=[any_spec] * 5 + [vmem, vmem],
        out_specs=(any_spec,) * 3,
        scratch_shapes=scratch,
        compiler_params=pltpu.CompilerParams(
            collective_id=0, has_side_effects=True, vmem_limit_bytes=67043328
        ),
        name="attention_backward",
    )(q, k, v, o, g, lp, ids)
    return pl.pallas_call(
        publish,
        out_shape=shapes,
        in_specs=[any_spec] * 3,
        out_specs=(any_spec,) * 3,
        scratch_shapes=[
            pltpu.VMEM((TOK, HEADS * D), BF16),
            pltpu.VMEM((TOK, GROUPS * D), BF16),
            pltpu.VMEM((TOK, GROUPS * D), BF16),
            dma((3,)),
            dma((3,)),
        ],
        name="publish",
    )(*grads)


def solution(mesh):
    tokens = ("blk", "uly")
    row = P(tokens, None)
    in_specs = (row, row, row, row, row, P(tokens, None, None), P(tokens))
    return jax.shard_map(
        per_device, mesh=mesh, in_specs=in_specs, out_specs=(row, row, row), check_vma=False
    )
```

```python
import math

import jax
import jax.numpy as jnp
from jax import lax
from jax.experimental import pallas as pl
from jax.experimental.pallas import tpu as pltpu
from jax.sharding import PartitionSpec as P

D = 128
HEADS = 16
GROUPS = 8
TOK = 128
ROWS = TOK * GROUPS
CH = 256
NCH = ROWS // CH
NY = 4
QB = 512
LOG2E = math.log2(math.e)
SCALE = 1.0 / math.sqrt(D)
MESH = pl.DeviceIdType.MESH
F32 = jnp.float32
BF16 = jnp.bfloat16


def mo(value, unit):
    return pl.multiple_of(value, unit)


def kernel(
    q_in, k_in, v_in, o_in, g_in, lp_in, id_in,
    q_out, k_out, v_out,
    Q, G, KV, ST, IDT, IDR, IDC,
    o_s, g_s, st_src, id_src, PKV, PQ, PG,
    DQ, ACC0, ACC1, ACC2,
    S2, R2, S1, R1, SO, SQ, XQ, XKV,
    loc, d2d_send, d2d_recv, yo_send, yo_recv,
    st_send, st_recv, id_send, id_recv,
    hop_send, hop_recv, ret_send, ret_recv,
    oq_send, oq_recv, okv_send, okv_recv, fwd_send, fwd_recv, lout,
):
    me = lax.axis_index("uly")
    blk = lax.axis_index("blk")
    nblk = lax.axis_size("blk")
    nxt = lax.rem(blk + 1, nblk)
    prv = lax.rem(blk + nblk - 1, nblk)
    y = me // 2
    core = lax.rem(me, 2)
    mate = me + 1 - 2 * core

    def rcopy(src, dst, ss, rs, p, b):
        return pltpu.make_async_remote_copy(
            src_ref=src, dst_ref=dst, send_sem=ss, recv_sem=rs,
            device_id=(p, b), device_id_type=MESH,
        )

    def peer(d):
        return lax.rem(me + d, GROUPS)

    def each_peer(f):
        def body(d, _):
            f(peer(d))
            return 0

        lax.fori_loop(1, GROUPS, body, 0)

    pair = y // 2

    def chip(k):
        step = k + (k // 2) * (5 - 2 * k)
        return lax.rem(y + (1 - 2 * lax.rem(y, 2)) * step + NY, NY)

    def rows_of(u):
        return pl.ds(mo(u * TOK, TOK), TOK)

    def chunk(c):
        return pl.ds(mo(c * CH, CH), CH)

    def wide(g):
        return pl.ds(mo(g * 2 * D, 2 * D), 2 * D)

    def narrow(g):
        return pl.ds(mo(g * D, D), D)

    cp_g = pltpu.make_async_copy(g_in, g_s, loc.at[0])
    cp_o = pltpu.make_async_copy(o_in, o_s, loc.at[1])

    own = [
        pltpu.make_async_copy(k_in.at[:, narrow(me)], KV.at[0, rows_of(me), 0:D], loc.at[2]),
        pltpu.make_async_copy(v_in.at[:, narrow(me)], KV.at[0, rows_of(me), D : 2 * D], loc.at[3]),
        pltpu.make_async_copy(q_in.at[:, wide(me)], Q.at[rows_of(me), :], loc.at[4]),
        pltpu.make_async_copy(g_in.at[:, wide(me)], G.at[rows_of(me), :], loc.at[5]),
    ]

    barrier = pltpu.get_barrier_semaphore()

    def greet(d, _):
        pl.semaphore_signal(barrier, inc=1, device_id=(peer(d), blk), device_id_type=MESH)
        return 0

    lax.fori_loop(1, GROUPS, greet, 0)
    pl.semaphore_signal(barrier, inc=1, device_id=(me, nxt), device_id_type=MESH)
    pl.semaphore_signal(barrier, inc=1, device_id=(me, prv), device_id_type=MESH)

    for cp in own:
        cp.start()
    cp_g.start()
    cp_o.start()
    id_src[...] = jnp.broadcast_to(id_in[...].astype(F32), (8, TOK))

    pl.semaphore_wait(barrier, GROUPS + 1)

    def source(kind, g):
        cols = narrow(g) if kind < 2 else wide(g)
        return (k_in, v_in, q_in, g_in)[kind].at[:, cols]

    def held(kind, t):
        return (PKV.at[t, :, 0:D], PKV.at[t, :, D : 2 * D], PQ.at[t], PG.at[t])[kind]

    def final(kind, u):
        rows = rows_of(u)
        return (
            KV.at[0, rows, 0:D], KV.at[0, rows, D : 2 * D], Q.at[rows, :], G.at[rows, :]
        )[kind]

    def mate_copy(kind, t, here, there, same):
        src = source(kind, 2 * t + lax.rem(there, 2))
        dst = final(kind, here) if same else held(kind, t)
        return rcopy(src, dst, d2d_send.at[kind, t], d2d_recv.at[kind, t], mate, blk)

    def mate_send(kind, k):
        return mate_copy(kind, chip(k), me, mate, k == 0)

    def mate_recv(kind, k):
        return mate_copy(kind, chip(k), mate, me, k == 0)

    for k in range(NY):
        mate_send(0, k).start()
        mate_send(1, k).start()

    def id_copy(p, src_i):
        return rcopy(id_src, IDT.at[src_i], id_send.at[p], id_recv.at[src_i], p, blk)

    def st_copy(p, src_i):
        return rcopy(st_src.at[p], ST.at[src_i], st_send.at[p], st_recv.at[src_i], p, blk)

    each_peer(lambda p: id_copy(p, me).start())

    def y_copy(kind, part, t, s):
        g = 2 * t + core
        u = 2 * s + (core if part == 0 else 1 - core)
        src = source(kind, g) if part == 0 else held(kind, t)
        return rcopy(
            src, final(kind, u), yo_send.at[kind, part, t], yo_recv.at[kind, part, s], g, blk
        )

    def hop_copy(slot, c):
        rows = chunk(c)
        return rcopy(
            KV.at[slot, rows, :], KV.at[slot + 1, rows, :],
            hop_send.at[slot, c], hop_recv.at[slot, c], me, nxt,
        )

    def ids_hop(slot):
        return rcopy(
            IDR.at[slot], IDR.at[slot + 1], hop_send.at[slot, NCH], hop_recv.at[slot, NCH], me, nxt
        )

    for k in range(1, NY):
        y_copy(0, 0, chip(k), y).start()
        y_copy(1, 0, chip(k), y).start()
    for kind in (2, 3):
        for k in range(NY):
            mate_send(kind, k).start()
    for k in range(1, NY):
        for kind in (0, 1):
            mate_recv(kind, k).wait_recv()
            y_copy(kind, 1, chip(k), y).start()
    own[0].wait()
    own[1].wait()
    mate_recv(0, 0).wait_recv()
    mate_recv(1, 0).wait_recv()
    hop_copy(0, chip(0)).start()
    for near in ((1, 2), (3,)):
        for k in near:
            for kind in (2, 3):
                y_copy(kind, 0, chip(k), y).start()
        for k in near:
            for kind in (2, 3):
                mate_recv(kind, k).wait_recv()
                y_copy(kind, 1, chip(k), y).start()

    IDT[me] = id_src[...]
    each_peer(lambda p: id_copy(me, p).wait_recv())
    IDR[0] = IDT[:, 0, :]

    def columns_of(slot):
        for s in range(GROUPS):
            tile = jnp.broadcast_to(IDR[slot, s : s + 1, :], (TOK, TOK))
            IDC[slot, s * TOK : (s + 1) * TOK, :] = tile.T

    ids_hop(0).start()
    for k in range(1, NY):
        for kind in (0, 1):
            for part in (0, 1):
                y_copy(kind, part, y, chip(k)).wait_recv()
        hop_copy(0, chip(k)).start()

    a, b = lp_in[:, 0, :], lp_in[:, 1, :]
    top = jnp.maximum(a, b)
    lse = (top + jnp.log(jnp.exp(a - top) + jnp.exp(b - top))) * LOG2E
    cp_g.wait()
    cp_o.wait()
    lane = lax.broadcasted_iota(jnp.int32, (TOK, D), 1)

    def delta_step(h, acc):
        cols = narrow(h)
        total = jnp.sum(g_s[:, cols].astype(F32) * o_s[:, cols].astype(F32), axis=1, keepdims=True)
        return jnp.where(lane == h, total, acc)

    deltas = lax.fori_loop(0, HEADS, delta_step, jnp.zeros((TOK, D), F32)).T
    for g in range(GROUPS):
        st_src[g] = jnp.concatenate(
            [lse[2 * g : 2 * g + 2], deltas[2 * g : 2 * g + 2], jnp.zeros((4, TOK), F32)], axis=0
        )
    ST[me] = st_src[me]
    each_peer(lambda p: st_copy(p, me).start())

    ids_hop(0).wait_recv()
    ids_hop(1).start()
    for k in range(2):
        hop_copy(0, chip(k)).wait_recv()
        hop_copy(1, chip(k)).start()

    columns_of(0)
    columns_of(1)
    DQ[...] = jnp.zeros_like(DQ)
    ACC0[...] = jnp.zeros_like(ACC0)
    ACC1[...] = jnp.zeros_like(ACC1)
    ACC2[...] = jnp.zeros_like(ACC2)

    def tile(slot, c, qb, acc, causal, depth):
        krows = pl.ds(mo(c * depth, depth), depth)
        qrows = pl.ds(mo(qb * QB, QB), QB)
        kt = KV[slot, krows, 0:D]
        vt = KV[slot, krows, D : 2 * D]
        idk = IDC[slot, krows, :]
        nq = QB // TOK
        first = qb * nq

        def row(r):
            return jnp.concatenate([ST[first + i, r : r + 1, :] for i in range(nq)], axis=1)

        idq = jnp.concatenate([IDR[0, pl.ds(first + i, 1), :] for i in range(nq)], axis=1)
        allowed = jnp.concatenate([idk] * nq, axis=1) == idq
        if causal:
            kpos = lax.broadcasted_iota(jnp.int32, (depth, QB), 0) + c * depth
            qpos = lax.broadcasted_iota(jnp.int32, (depth, QB), 1) + qb * QB
            allowed = allowed & (kpos <= qpos)
        dk = jnp.zeros((depth, D), F32)
        dv = jnp.zeros((depth, D), F32)
        turned = kt.T
        for h in range(2):
            cols = slice(h * D, (h + 1) * D)
            qt = Q[qrows, cols]
            gt = G[qrows, cols]
            s = lax.dot_general(kt, qt, (((1,), (1,)), ((), ())), preferred_element_type=F32)
            w = jnp.where(allowed, jnp.exp2(s * (SCALE * LOG2E) - row(h)), 0.0)
            dp = lax.dot_general(vt, gt, (((1,), (1,)), ((), ())), preferred_element_type=F32)
            sg = (w * (dp - row(2 + h))).astype(BF16)
            dv = dv + jnp.dot(w.astype(BF16), gt, preferred_element_type=F32)
            dk = dk + jnp.dot(sg, qt, preferred_element_type=F32)
            DQ[cols, qrows] += jnp.dot(turned, sg, preferred_element_type=F32)
        acc[krows, 0:D] += dk
        acc[krows, D : 2 * D] += dv

    def wait_qg(k):
        for kind in (2, 3):
            y_copy(kind, 0, y, chip(k)).wait_recv()
            y_copy(kind, 1, y, chip(k)).wait_recv()

    def own_tiles(qb, count):
        lax.fori_loop(0, count, lambda c, _: (tile(0, c, qb, ACC0, True, QB), 0)[1], 0)

    def ret_copy(stage, c):
        rows = chunk(c)
        src, dst = (S2, R2) if stage == 0 else (S1, R1)
        return rcopy(
            src.at[rows, :], dst.at[rows, :], ret_send.at[stage, c], ret_recv.at[stage, c], me, prv
        )

    scales = jnp.where(lax.broadcasted_iota(jnp.int32, (CH, 2 * D), 1) < D, SCALE, 1.0)

    each_peer(lambda p: st_copy(me, p).wait_recv())
    own[2].wait()
    own[3].wait()
    mate_recv(2, 0).wait_recv()
    mate_recv(3, 0).wait_recv()
    wait_qg(1)
    own_tiles(pair, pair + 1)
    for k in range(2, NY):
        hop_copy(0, chip(k)).wait_recv()
        hop_copy(1, chip(k)).start()

    def two_tiles(c, first, stop):
        lax.fori_loop(first, stop, lambda qb, _: (tile(2, c, qb, ACC2, False, CH), 0)[1], 0)

    def send_two(c):
        S2[chunk(c), :] = (ACC2[chunk(c), :] * scales).astype(BF16)
        ret_copy(0, c).start()

    ids_hop(1).wait_recv()
    columns_of(2)
    hop_copy(1, chip(0)).wait_recv()
    two_tiles(chip(0), pair, pair + 1)

    @pl.when(pair == 0)
    def _():
        send_two(chip(0))

    wait_qg(2)
    wait_qg(3)

    def hop_one(half):
        lax.fori_loop(0, ROWS // QB, lambda qb, _: (tile(1, half, qb, ACC1, False, QB), 0)[1], 0)

    def pass_on(c):
        ret_copy(0, c).wait_recv()
        S1[chunk(c), :] = (ACC1[chunk(c), :] * scales + R2[chunk(c), :].astype(F32)).astype(BF16)
        ret_copy(1, c).start()

    def hop_two(k, _):
        c = chip(k)
        late = k // 2

        @pl.when(k > 0)
        def _():
            hop_copy(1, c).wait_recv()

        two_tiles(c, 0, pair + (2 - 2 * pair) * late + lax.rem(k, 2) * (1 - late))

        @pl.when(pair + k > 0)
        def _():
            send_two(c)

        @pl.when(lax.rem(k, 2) == 1)
        def _():
            hop_one(1 - pair + (2 * pair - 1) * late)

        return 0

    lax.fori_loop(0, NCH, hop_two, 0)

    def okv_copy(t, s):
        return rcopy(
            SO.at[chunk(t), :], XKV.at[s], okv_send.at[t], okv_recv.at[s], 2 * t + core, blk
        )

    def oq_copy(t, s):
        return rcopy(
            SQ.at[chunk(t), :], XQ.at[s], oq_send.at[t], oq_recv.at[s], 2 * t + core, blk
        )

    def total(c):
        ret_copy(1, c).wait_recv()
        return (ACC0[chunk(c), :] * scales + R1[chunk(c), :].astype(F32)).astype(BF16)

    def out_chunk(k):
        c = chip(k)
        SO[chunk(c), :] = total(c)
        okv_copy(c, y).start()

    pass_on(chip(2))
    pass_on(chip(3))
    pass_on(chip(1))
    pass_on(chip(0))
    own_tiles(1 - pair, 2 - pair)

    mine = pl.ds(mo(core * TOK, TOK), TOK)
    theirs = pl.ds(mo((1 - core) * TOK, TOK), TOK)

    def forward(s, kind, owner):
        g = 2 * s + lax.rem(owner, 2)
        if kind == 0:
            src, dst = XQ.at[s, theirs, :], q_out.at[:, wide(g)]
        elif kind == 1:
            src, dst = XKV.at[s, theirs, 0:D], k_out.at[:, narrow(g)]
        else:
            src, dst = XKV.at[s, theirs, D : 2 * D], v_out.at[:, narrow(g)]
        return rcopy(src, dst, fwd_send.at[kind, s], fwd_recv.at[kind, s], mate, blk)

    def keep(s, kind):
        g = 2 * s + core
        if kind == 0:
            src, dst = XQ.at[s, mine, :], q_out.at[:, wide(g)]
        elif kind == 1:
            src, dst = XKV.at[s, mine, 0:D], k_out.at[:, narrow(g)]
        else:
            src, dst = XKV.at[s, mine, D : 2 * D], v_out.at[:, narrow(g)]
        return pltpu.make_async_copy(src, dst, lout.at[kind, s])

    def deliver(s, kind):
        forward(s, kind, me).start()
        keep(s, kind).start()

    def turn(c):
        return (DQ[:, chunk(c)] * SCALE).T.astype(BF16)

    def send_q(k, _):
        c = chip(k)
        SQ[chunk(c), :] = turn(c)
        oq_copy(c, y).start()
        return 0

    lax.fori_loop(1, NY, send_q, 0)
    XQ[y] = turn(y)
    deliver(y, 0)
    out_chunk(2)
    out_chunk(3)
    out_chunk(1)

    def arrivals(k, _):
        s = chip(k)
        oq_copy(y, s).wait_recv()
        deliver(s, 0)
        return 0

    lax.fori_loop(1, NY, arrivals, 0)

    def arrivals_kv(k, _):
        s = chip(k)
        okv_copy(y, s).wait_recv()
        deliver(s, 1)
        deliver(s, 2)
        return 0

    lax.fori_loop(2, NY, arrivals_kv, 0)
    XKV[y] = total(y)
    deliver(y, 1)
    deliver(y, 2)
    arrivals_kv(1, 0)

    def drain_small(p):
        id_copy(p, me).wait_send()
        st_copy(p, me).wait_send()

    each_peer(drain_small)
    for slot in range(2):
        ids_hop(slot).wait_send()
    for stage in range(2):
        for c in range(NCH):
            hop_copy(stage, c).wait_send()
            ret_copy(stage, c).wait_send()
    for k in range(NY):
        for kind in range(4):
            mate_send(kind, k).wait_send()
            if k > 0:
                y_copy(kind, 0, chip(k), y).wait_send()
                y_copy(kind, 1, chip(k), y).wait_send()
        if k > 0:
            oq_copy(chip(k), y).wait_send()
            okv_copy(chip(k), y).wait_send()

    def drain_out(s, _):
        for kind in range(3):
            forward(s, kind, me).wait_send()
            keep(s, kind).wait()
            forward(s, kind, mate).wait_recv()
        return 0

    lax.fori_loop(0, NY, drain_out, 0)


def publish(q_in, k_in, v_in, q_out, k_out, v_out, q_s, k_s, v_s, read, write):
    moves = ((q_in, q_s, q_out), (k_in, k_s, k_out), (v_in, v_s, v_out))
    reads, writes = [], []
    for i, (a, b, c) in enumerate(moves):
        for half in range(2):
            rows = pl.ds(half * (TOK // 2), TOK // 2)
            n = 2 * i + half
            reads.append(pltpu.make_async_copy(a.at[rows, :], b.at[rows, :], read.at[n]))
            writes.append(pltpu.make_async_copy(b.at[rows, :], c.at[rows, :], write.at[n]))
    for cp in reads:
        cp.start()
    for cp, back in zip(reads, writes):
        cp.wait()
        back.start()
    for cp in writes:
        cp.wait()


def per_device(q, k, v, o, g, lp, ids):
    lp = lp.transpose(1, 2, 0)
    ids = ids.reshape(1, TOK)
    any_spec = pl.BlockSpec(memory_space=pl.ANY)
    vmem = pl.BlockSpec(memory_space=pltpu.VMEM)
    dma = pltpu.SemaphoreType.DMA
    slab = pltpu.VMEM((ROWS, 2 * D), BF16)
    acc = pltpu.VMEM((ROWS, 2 * D), F32)
    block = pltpu.VMEM((NY, TOK, 2 * D), BF16)
    scratch = [
        slab,
        slab,
        pltpu.VMEM((3, ROWS, 2 * D), BF16),
        pltpu.VMEM((GROUPS, 8, TOK), F32),
        pltpu.VMEM((GROUPS, 8, TOK), F32),
        pltpu.VMEM((3, GROUPS, TOK), F32),
        pltpu.VMEM((3, ROWS, TOK), F32),
        pltpu.VMEM((TOK, HEADS * D), BF16),
        pltpu.VMEM((TOK, HEADS * D), BF16),
        pltpu.VMEM((GROUPS, 8, TOK), F32),
        pltpu.VMEM((8, TOK), F32),
        block, block, block,
        pltpu.VMEM((2 * D, ROWS), F32),
        acc, acc, acc,
        slab, slab, slab, slab, slab, slab,
        pltpu.VMEM((NY, CH, 2 * D), BF16),
        pltpu.VMEM((NY, CH, 2 * D), BF16),
        dma((6,)),
        dma((4, NY)), dma((4, NY)),
        dma((4, 2, NY)), dma((4, 2, NY)),
        dma((GROUPS,)), dma((GROUPS,)),
        dma((GROUPS,)), dma((GROUPS,)),
        dma((2, NCH + 1)), dma((2, NCH + 1)),
        dma((2, NCH)), dma((2, NCH)),
        dma((NY,)), dma((NY,)), dma((NY,)), dma((NY,)),
        dma((3, NY)), dma((3, NY)), dma((3, NY)),
    ]
    shapes = (
        jax.ShapeDtypeStruct((TOK, HEADS * D), BF16),
        jax.ShapeDtypeStruct((TOK, GROUPS * D), BF16),
        jax.ShapeDtypeStruct((TOK, GROUPS * D), BF16),
    )
    grads = pl.pallas_call(
        kernel,
        out_shape=shapes,
        in_specs=[any_spec] * 5 + [vmem, vmem],
        out_specs=(any_spec,) * 3,
        scratch_shapes=scratch,
        compiler_params=pltpu.CompilerParams(
            collective_id=0, has_side_effects=True, vmem_limit_bytes=67043328
        ),
        name="attention_backward",
    )(q, k, v, o, g, lp, ids)
    return pl.pallas_call(
        publish,
        out_shape=shapes,
        in_specs=[any_spec] * 3,
        out_specs=(any_spec,) * 3,
        scratch_shapes=[
            pltpu.VMEM((TOK, HEADS * D), BF16),
            pltpu.VMEM((TOK, GROUPS * D), BF16),
            pltpu.VMEM((TOK, GROUPS * D), BF16),
            dma((6,)),
            dma((6,)),
        ],
        name="publish",
    )(*grads)


def solution(mesh):
    tokens = ("blk", "uly")
    row = P(tokens, None)
    in_specs = (row, row, row, row, row, P(tokens, None, None), P(tokens))
    return jax.shard_map(
        per_device, mesh=mesh, in_specs=in_specs, out_specs=(row, row, row), check_vma=False
    )
```
